32 devices in a mesh: sp: 2 (over core), py: 4 (over z), pz: 4 (over y, x).
Axes of the slice: x: 2, y: 2, z: 4, core: 2. Of those that a mesh axis runs over, the one named last changes fastest.
Arguments:
- concentration: float32 [8, 128, 128, 128], P('sp', 'py', 'pz'), may hold values from -1 to 1.1
- mobility: float32 [8, 8], replicated, may hold values from 0.1 to 0.6
- kappa: float32 [8], replicated, may hold values from 0.5 to 2
- well_depth: float32 [8], P('sp'), may hold values from 0.5 to 2
Outputs:
- updated: float32 [8, 128, 128, 128], P('sp', 'py', 'pz')
The draws below stay inside these ranges and needn't reach their ends.
All inputs are finite; a program needn't handle non-finite values.
Results may differ from the reference program's by a relative error of at most 0.000084.
Values sent between devices are 32-bit elements; how exact they have to be, the bound alone decides.
No kernel may reach another device: no remote copies, remote signals or barrier semaphores. Data moves between devices by JAX's collectives and lax.ppermute only.
A program may use at most 128 MiB of HBM per device.

```python
import math
import jax
import jax.numpy as jnp
from jax import lax

S = 8
NX = 128
NY = 128
NZ = 128


def draw_concentration(key, part):
    first = jax.random.fold_in(jax.random.fold_in(key, 11), 0)
    base = jax.random.uniform(first, (S, NX, NY, NZ), jnp.float32, -1.0, 1.0)
    return base


def level_of(own_key, extent, cuts, least, top_value):
    factor_of = 1.0
    for position, shards_of in cuts:
        draws = jax.random.uniform(jax.random.fold_in(jax.random.fold_in(own_key, 6), position), (shards_of,), jnp.float32, least / len(cuts), top_value / len(cuts))
        factor_of = factor_of * jnp.repeat(jnp.exp(draws), extent[position] // shards_of).reshape((-1,) + (1,) * (len(extent) - 1 - position))
    return factor_of


def setup_inputs(seed: int = 0) -> dict:
    seeds = jax.random.split(jax.random.key(seed), 5)
    return {
        "concentration": draw_concentration(jax.random.fold_in(seeds[4], 71), 0),
        "mobility": jnp.clip(jax.random.uniform(seeds[1], (S, S), jnp.float32, 0.1, 0.6), 0.1, 0.6),
        "kappa": jnp.clip(jnp.exp(jax.random.uniform(seeds[2], (S,), jnp.float32, math.log(0.5), math.log(2.0))), 0.5, 2.0),
        "well_depth": jnp.clip(jnp.exp(math.log(2.0) - 1.3862944 * jax.random.uniform(seeds[3], (S,), jnp.float32) ** level_of(seeds[3], (S,), ((0, 2),), -0.2, 0.2)), 0.5, 2.0),
    }


def wave_square(count):
    modes = jnp.arange(count, dtype=jnp.int32)
    freq = jnp.where(modes < count // 2, modes, modes - count).astype(jnp.float32)
    return (2.0 * math.pi * freq / count) ** 2


def reference(concentration, mobility, kappa, well_depth):
    conc = concentration
    bulk = well_depth[:, None, None, None] * (conc * conc * conc - conc)
    c_hat = jnp.fft.fftn(conc, axes=(1, 2, 3))
    bulk_hat = jnp.fft.fftn(bulk, axes=(1, 2, 3))
    ksq = wave_square(NX)[:, None, None] + wave_square(NY)[None, :, None] + wave_square(NZ)[None, None, :]
    drive = bulk_hat + kappa[:, None, None, None] * ksq[None] * c_hat
    mix_real = jnp.einsum("ij,jxyz->ixyz", mobility, jnp.real(drive), precision=lax.Precision.HIGHEST)
    mix_imag = jnp.einsum("ij,jxyz->ixyz", mobility, jnp.imag(drive), precision=lax.Precision.HIGHEST)
    mix = mix_real + 1j * mix_imag
    stiff = 0.5 * (jnp.diagonal(mobility) * kappa)[:, None, None, None] * (ksq * ksq)[None]
    new_hat = (c_hat * (1.0 + stiff) - 0.5 * ksq[None] * mix) / (1.0 + stiff)
    updated = jnp.real(jnp.fft.ifftn(new_hat, axes=(1, 2, 3)))
    return updated.astype(jnp.float32)
```

```python
import functools
import math

import jax
import jax.numpy as jnp
import numpy as np
from jax import lax
from jax.experimental import pallas as pl
from jax.experimental.pallas import tpu as pltpu
from jax.sharding import PartitionSpec as P

CHUNKS = 2
ROWS = 128
BF16 = jnp.bfloat16
F32 = jnp.float32


def cas_table(count):
    modes = np.arange(count)
    angle = 2.0 * np.pi * (modes[:, None] * modes[None, :] % count) / count
    return np.cos(angle) + np.sin(angle)


def halves(table):
    high = table.astype(BF16)
    low = (table - high.astype(np.float64)).astype(BF16)
    return high, low


def wave_square(index, count):
    freq = jnp.where(index < count // 2, index, index - count).astype(F32)
    return (2.0 * math.pi * freq / count) ** 2


def split(x):
    high = x.astype(BF16)
    return high, (x - high.astype(F32)).astype(BF16)


def dot(a, b, dims=((1,), (0,))):
    return lax.dot_general(a, b, (dims, ((), ())), preferred_element_type=F32)


def left_apply(table, x):
    high, low = split(x)
    return dot(table, jnp.concatenate([high, high, low], axis=0))


def z_forward(c_ref, w_ref, t_ref, *out_refs, rows_y, chunks):
    lanes = w_ref.shape[0]
    table = t_ref[...]
    weight = w_ref[...]
    width = out_refs[0].shape[2]
    dests = t_ref.shape[0] // (width * chunks)

    def body(y, carry):
        c = c_ref[pl.ds(y, lanes, stride=rows_y), :]
        bulk = weight * (c * c * c - c)
        for f, x in enumerate((c, bulk)):
            high, low = split(x)
            res = dot(table, jnp.concatenate([high, high, low], axis=1), ((1,), (1,)))
            for dest in range(dests):
                for n in range(chunks):
                    first = (dest * chunks + n) * width
                    out_refs[n * dests + dest][f, y] = res[first : first + width]
        return carry

    lax.fori_loop(0, rows_y, body, 0, unroll=4)


def y_forward(*refs, rows_y, count_pz):
    x_refs, t_ref, out_refs = refs[:count_pz], refs[count_pz], refs[count_pz + 1 :]
    table = t_ref[...]
    fields, width, narrow, _ = out_refs[0].shape

    def body(kz, carry):
        for f in range(fields):
            x = jnp.concatenate(
                [
                    ref[pl.ds(f * rows_y * width + kz, rows_y, stride=width), :]
                    for ref in x_refs
                ],
                axis=0,
            )
            res = left_apply(table, x)
            for dest, ref in enumerate(out_refs):
                ref[f, kz] = res[dest * narrow : (dest + 1) * narrow]
        return carry

    lax.fori_loop(0, width, body, 0, unroll=2)


def x_forward(*refs, sources):
    x_refs = refs[:sources]
    high_ref, low_ref, row_ref, col_ref, kappa_ref, mob_ref, *out_refs = refs[sources:]
    rows = x_refs[0].shape[1]
    species, full_x = out_refs[0].shape[0], out_refs[0].shape[2]

    def body(block, carry):
        at = pl.ds(pl.multiple_of(block * ROWS, ROWS), ROWS)
        spectra = []
        for f in range(2):
            x = jnp.concatenate([ref[f, at, :] for ref in x_refs], axis=1)
            high, low = split(x)
            spectra.append(
                dot(high, high_ref[...]) + dot(low, high_ref[...]) + dot(high, low_ref[...])
            )
        ksq = row_ref[at, :] + col_ref[...]
        drive = []
        for s in range(species):
            own = slice(s * full_x, (s + 1) * full_x)
            drive.append(spectra[1][:, own] + (kappa_ref[s] * ksq) * spectra[0][:, own])
        for d, ref in enumerate(out_refs):
            for i in range(species):
                total = mob_ref[d, i, 0] * drive[0]
                for s in range(1, species):
                    total = total + mob_ref[d, i, s] * drive[s]
                ref[i, at, :] = total
        return carry

    lax.fori_loop(0, rows // ROWS, body, 0)


def x_inverse(*refs, shares):
    mix_refs = refs[:shares]
    high_ref, low_ref, row_ref, col_ref, stiff_ref, *out_refs = refs[shares:]
    species, rows, _ = mix_refs[0].shape
    lanes = out_refs[0].shape[1]

    def body(block, carry):
        at = pl.ds(pl.multiple_of(block * ROWS, ROWS), ROWS)
        ksq = row_ref[at, :] + col_ref[...]
        half = 0.5 * ksq
        square = ksq * ksq
        parts = []
        for i in range(species):
            mix = mix_refs[0][i, at, :]
            for ref in mix_refs[1:]:
                mix = mix + ref[i, at, :]
            parts.append(half * mix / (1.0 + stiff_ref[i] * square))
        high, low = split(jnp.concatenate(parts, axis=1))
        turned = ((1,), (1,))
        res = (
            dot(high, high_ref[...], turned)
            + dot(low, high_ref[...], turned)
            + dot(high, low_ref[...], turned)
        )
        for dest, ref in enumerate(out_refs):
            ref[at, :] = res[:, dest * lanes : (dest + 1) * lanes]
        return carry

    lax.fori_loop(0, rows // ROWS, body, 0)


def y_inverse(*refs, count_py):
    x_refs, t_ref, out_refs = refs[:count_py], refs[count_py], refs[count_py + 1 :]
    table = t_ref[...]
    width, rows_y, _ = out_refs[0].shape

    def body(kz, carry):
        x = jnp.concatenate([ref[kz] for ref in x_refs], axis=0)
        res = left_apply(table, x)
        for dest, ref in enumerate(out_refs):
            ref[kz] = res[dest * rows_y : (dest + 1) * rows_y]
        return carry

    lax.fori_loop(0, width, body, 0, unroll=4)


def z_inverse(*refs, rows_y, count_pz, scale):
    *x_refs, c_ref, t_ref, out_ref = refs
    lanes = x_refs[0].shape[1]
    width = x_refs[0].shape[0] // rows_y
    chunks = len(x_refs) // count_pz
    table = t_ref[...]

    def body(y, carry):
        x = jnp.concatenate(
            [
                x_refs[n * count_pz + src][pl.ds(y, width, stride=rows_y), :]
                for src in range(count_pz)
                for n in range(chunks)
            ],
            axis=0,
        )
        high, low = split(x.T)
        res = dot(jnp.concatenate([high, high, low], axis=1), table)
        at = pl.ds(y, lanes, stride=rows_y)
        out_ref[at, :] = c_ref[at, :] - scale * res
        return carry

    lax.fori_loop(0, rows_y, body, 0, unroll=4)


VMEM = pl.BlockSpec(memory_space=pltpu.VMEM)
SMEM = pl.BlockSpec(memory_space=pltpu.SMEM)


def call(body, shapes, ins, specs=None, **kwargs):
    many = isinstance(shapes, list)
    listed = shapes if many else [shapes]
    out = pl.pallas_call(
        functools.partial(body, **kwargs),
        out_shape=[jax.ShapeDtypeStruct(s, F32) for s in listed],
        in_specs=specs or [VMEM] * len(ins),
        out_specs=[VMEM] * len(listed),
        name=body.__name__,
    )(*ins)
    return out if many else out[0]


def setting(concentration, mobility, kappa):
    species = concentration.shape[0]
    count_sp = lax.axis_size("sp")
    me = lax.axis_index("sp")
    own_kappa = lax.dynamic_slice_in_dim(kappa, me * species, species)
    columns = lax.dynamic_slice_in_dim(mobility, me * species, species, 1)
    shares = jnp.stack(
        [
            lax.dynamic_slice_in_dim(columns, (me + d) % count_sp * species, species, 0)
            for d in range(count_sp)
        ]
    )
    diagonal = lax.dynamic_slice_in_dim(jnp.diagonal(mobility), me * species, species)
    return own_kappa, shares, 0.5 * diagonal * own_kappa


def exchange(shares):
    count_sp = len(shares)
    out = [shares[0]]
    for d in range(1, count_sp):
        ring = [(i, (i + d) % count_sp) for i in range(count_sp)]
        out.append(lax.ppermute(shares[d], "sp", ring))
    return out


def swap(x, axis):
    return lax.all_to_all(x, axis, split_axis=0, concat_axis=0, tiled=True)


def hand_round(blocks, axis):
    count = len(blocks)
    out = [blocks[0]]
    for d in range(1, count):
        out.append(lax.ppermute(blocks[d], axis, [(i, (i - d) % count) for i in range(count)]))
    return out


def turn(table, dimension, axis, step):
    count, me = lax.axis_size(axis), lax.axis_index(axis)
    size = table.shape[dimension]
    order = np.arange(2 * count) * step % count
    places = (order[:, None] * (size // count) + np.arange(size // count)).reshape(-1)
    wide = jnp.take(table, places, axis=dimension)
    return lax.dynamic_slice_in_dim(wide, me * step % count * (size // count), size, dimension)


def dense(concentration, mobility, kappa, well_depth):
    species, rows_x, rows_y, depth = concentration.shape
    count_sp, count_py, count_pz = (lax.axis_size(a) for a in ("sp", "py", "pz"))
    full_x, full_y = rows_x * count_py, rows_y * count_pz
    lanes = species * rows_x
    narrow = full_y // count_py
    own_z = depth // count_pz
    chunks = CHUNKS
    width = own_z // chunks
    rows = width * narrow

    z_high, z_low = halves(cas_table(depth))
    y_high, y_low = halves(cas_table(full_y))
    z_left = turn(np.concatenate([z_high, z_low, z_high], axis=1), 0, "pz", -1)
    z_right = [turn(t, 0, "pz", 1) for t in (z_high, z_low)]
    z_right = jnp.concatenate([*z_right, z_right[0]], axis=0)
    y_left = [turn(turn(t, 1, "pz", 1), 0, "py", -1) for t in (y_high, y_low)]
    y_left = jnp.concatenate([*y_left, y_left[0]], axis=1)
    y_back = [turn(turn(t, 1, "py", 1), 0, "pz", -1) for t in (y_high, y_low)]
    y_back = jnp.concatenate([*y_back, y_back[0]], axis=1)
    x_table = cas_table(full_x).reshape(count_py, 1, rows_x, 1, full_x)
    x_table = x_table * np.eye(species)[None, :, None, :, None]
    x_tables = halves(x_table.reshape(count_py * lanes, species * full_x))
    x_left = [turn(t, 0, "py", 1) for t in x_tables]
    x_back = [turn(t, 0, "py", -1) for t in x_tables]

    own_kappa, shares, stiff = setting(concentration, mobility, kappa)
    weight = jnp.broadcast_to(jnp.repeat(well_depth, rows_x)[:, None], (lanes, depth))
    flat = concentration.reshape(species * rows_x * rows_y, depth)
    ky = lax.axis_index("py") * narrow + jnp.arange(narrow, dtype=jnp.int32)
    ksq_x = wave_square(jnp.arange(full_x, dtype=jnp.int32), full_x)[None]

    spectra = call(
        z_forward,
        [(2, rows_y, width, lanes)] * (chunks * count_pz),
        (flat, weight, z_left),
        rows_y=rows_y,
        chunks=chunks,
    )
    moved = []
    for n in range(chunks):
        kz = lax.axis_index("pz") * own_z + n * width + jnp.arange(width, dtype=jnp.int32)
        ksq = wave_square(kz, depth)[:, None] + wave_square(ky, full_y)[None]
        ksq = jnp.broadcast_to(ksq.reshape(rows, 1), (rows, full_x))
        x = hand_round(spectra[n * count_pz : (n + 1) * count_pz], "pz")
        x = call(
            y_forward,
            [(2, width, narrow, lanes)] * count_py,
            (*[part.reshape(-1, lanes) for part in x], y_left),
            rows_y=rows_y,
            count_pz=count_pz,
        )
        x = hand_round(x, "py")
        mixes = call(
            x_forward,
            [(species, rows, full_x)] * count_sp,
            (*[part.reshape(2, rows, lanes) for part in x], *x_left, ksq, ksq_x, own_kappa, shares),
            [VMEM] * (count_py + 4) + [SMEM] * 2,
            sources=count_py,
        )
        mixes = exchange(mixes)
        x = call(
            x_inverse,
            [(rows, lanes)] * count_py,
            (*mixes, *x_back, ksq, ksq_x, stiff),
            [VMEM] * (count_sp + 4) + [SMEM],
            shares=count_sp,
        )
        x = hand_round(x, "py")
        x = call(
            y_inverse,
            [(width, rows_y, lanes)] * count_pz,
            (*[part.reshape(width, narrow, lanes) for part in x], y_back),
            count_py=count_py,
        )
        moved += [part.reshape(-1, lanes) for part in hand_round(x, "pz")]
    out = call(
        z_inverse,
        flat.shape,
        (*moved, flat, z_right),
        rows_y=rows_y,
        count_pz=count_pz,
        scale=1.0 / (full_x * full_y * depth),
    )
    return out.reshape(concentration.shape)


def contract(form, x, table):
    return jnp.einsum(form, x, table, precision=lax.Precision.HIGHEST)


def plain(concentration, mobility, kappa, well_depth):
    species, rows_x, rows_y, depth = concentration.shape
    count_py, count_pz = (lax.axis_size(a) for a in ("py", "pz"))
    full_x, full_y = rows_x * count_py, rows_y * count_pz
    narrow, own_z = full_y // count_py, depth // count_pz
    table_x, table_y, table_z = (jnp.asarray(cas_table(n), F32) for n in (full_x, full_y, depth))
    own_kappa, shares, stiff = setting(concentration, mobility, kappa)
    cube = concentration * concentration * concentration
    bulk = well_depth[:, None, None, None] * (cube - concentration)
    fields = jnp.stack([concentration, bulk])
    x = contract("fsxyz,kz->kfysx", fields, table_z)
    x = swap(x, "pz").reshape(count_pz, own_z, 2, rows_y, species, rows_x)
    x = contract("akfysx,qay->qfksx", x, table_y.reshape(full_y, count_pz, rows_y))
    x = swap(x, "py").reshape(count_py, narrow, 2, own_z, species, rows_x)
    x = contract("aqfksx,pax->fskqp", x, table_x.reshape(full_x, count_py, rows_x))
    kz = lax.axis_index("pz") * own_z + jnp.arange(own_z, dtype=jnp.int32)
    ky = lax.axis_index("py") * narrow + jnp.arange(narrow, dtype=jnp.int32)
    ksq_x = wave_square(jnp.arange(full_x, dtype=jnp.int32), full_x)
    ksq = wave_square(kz, depth)[:, None, None] + wave_square(ky, full_y)[:, None] + ksq_x
    drive = x[1] + own_kappa[:, None, None, None] * ksq * x[0]
    mixes = exchange([contract("skqp,is->ikqp", drive, shares[d]) for d in range(shares.shape[0])])
    x = 0.5 * ksq * sum(mixes) / (1.0 + stiff[:, None, None, None] * (ksq * ksq))
    x = swap(contract("skqp,xp->xqks", x, table_x), "py")
    x = x.reshape(count_py, rows_x, narrow, own_z, species)
    x = contract("axqks,yaq->yxks", x, table_y.reshape(full_y, count_py, narrow))
    x = swap(x, "pz").reshape(count_pz, rows_y, rows_x, own_z, species)
    x = contract("ayxks,zak->sxyz", x, table_z.reshape(depth, count_pz, own_z))
    return concentration - x * (1.0 / (full_x * full_y * depth))


def solution(mesh):
    def per_device(concentration, *rest):
        species, rows_x, rows_y, depth = concentration.shape
        full_x = rows_x * lax.axis_size("py")
        whole_tiles = [species * rows_x, full_x, depth]
        body = plain if any(n % 128 for n in whole_tiles) else dense
        return body(concentration, *rest)

    in_specs = (P("sp", "py", "pz", None), P(), P(), P("sp"))
    out_specs = P("sp", "py", "pz", None)
    return jax.shard_map(
        per_device, mesh=mesh, in_specs=in_specs, out_specs=out_specs, check_vma=False
    )
```

```python
import functools
import math

import jax
import jax.numpy as jnp
import numpy as np
from jax import lax
from jax.experimental import pallas as pl
from jax.experimental.pallas import tpu as pltpu
from jax.sharding import PartitionSpec as P

CHUNKS = 2
ROWS = 128
BF16 = jnp.bfloat16
F32 = jnp.float32


def cas_table(count):
    modes = np.arange(count)
    angle = 2.0 * np.pi * (modes[:, None] * modes[None, :] % count) / count
    return np.cos(angle) + np.sin(angle)


def halves(table):
    high = table.astype(BF16)
    low = (table - high.astype(np.float64)).astype(BF16)
    return high, low


def wave_square(index, count):
    freq = jnp.where(index < count // 2, index, index - count).astype(F32)
    return (2.0 * math.pi * freq / count) ** 2


def split(x):
    high = x.astype(BF16)
    return high, (x - high.astype(F32)).astype(BF16)


def dot(a, b, dims=((1,), (0,))):
    return lax.dot_general(a, b, (dims, ((), ())), preferred_element_type=F32)


def left_apply(table, x):
    high, low = split(x)
    return dot(table, jnp.concatenate([high, high, low], axis=0))


def z_forward(c_ref, w_ref, t_ref, *out_refs, rows_y, chunks):
    lanes = w_ref.shape[0]
    table = t_ref[...]
    weight = w_ref[...]
    width = out_refs[0].shape[2]
    dests = t_ref.shape[0] // (width * chunks)

    def body(y, carry):
        c = c_ref[pl.ds(y, lanes, stride=rows_y), :]
        bulk = weight * (c * c * c - c)
        for f, x in enumerate((c, bulk)):
            high, low = split(x)
            res = dot(table, jnp.concatenate([high, high, low], axis=1), ((1,), (1,)))
            for dest in range(dests):
                for n in range(chunks):
                    first = (dest * chunks + n) * width
                    out_refs[n * dests + dest][f, y] = res[first : first + width]
        return carry

    lax.fori_loop(0, rows_y, body, 0, unroll=4)


def y_forward(*refs, rows_y, count_pz):
    x_refs, t_ref, out_refs = refs[:count_pz], refs[count_pz], refs[count_pz + 1 :]
    table = t_ref[...]
    fields, width, narrow, _ = out_refs[0].shape

    def body(kz, carry):
        for f in range(fields):
            x = jnp.concatenate(
                [
                    ref[pl.ds(f * rows_y * width + kz, rows_y, stride=width), :]
                    for ref in x_refs
                ],
                axis=0,
            )
            res = left_apply(table, x)
            for dest, ref in enumerate(out_refs):
                ref[f, kz] = res[dest * narrow : (dest + 1) * narrow]
        return carry

    lax.fori_loop(0, width, body, 0, unroll=2)


def x_forward(*refs, sources):
    x_refs = refs[:sources]
    high_ref, low_ref, row_ref, col_ref, kappa_ref, mob_ref, *out_refs = refs[sources:]
    rows = x_refs[0].shape[1]
    species, full_x = out_refs[0].shape[0], out_refs[0].shape[2]

    def body(block, carry):
        at = pl.ds(pl.multiple_of(block * ROWS, ROWS), ROWS)
        spectra = []
        for f in range(2):
            x = jnp.concatenate([ref[f, at, :] for ref in x_refs], axis=1)
            high, low = split(x)
            spectra.append(
                dot(high, high_ref[...]) + dot(low, high_ref[...]) + dot(high, low_ref[...])
            )
        ksq = row_ref[at, :] + col_ref[...]
        drive = []
        for s in range(species):
            own = slice(s * full_x, (s + 1) * full_x)
            drive.append(spectra[1][:, own] + (kappa_ref[s] * ksq) * spectra[0][:, own])
        for d, ref in enumerate(out_refs):
            for i in range(species):
                total = mob_ref[d, i, 0] * drive[0]
                for s in range(1, species):
                    total = total + mob_ref[d, i, s] * drive[s]
                ref[i, at, :] = total
        return carry

    lax.fori_loop(0, rows // ROWS, body, 0)


def x_inverse(*refs, shares):
    mix_refs = refs[:shares]
    high_ref, low_ref, row_ref, col_ref, stiff_ref, *out_refs = refs[shares:]
    species, rows, _ = mix_refs[0].shape
    lanes = out_refs[0].shape[1]

    def body(block, carry):
        at = pl.ds(pl.multiple_of(block * ROWS, ROWS), ROWS)
        ksq = row_ref[at, :] + col_ref[...]
        half = 0.5 * ksq
        square = ksq * ksq
        parts = []
        for i in range(species):
            mix = mix_refs[0][i, at, :]
            for ref in mix_refs[1:]:
                mix = mix + ref[i, at, :]
            parts.append(half * mix / (1.0 + stiff_ref[i] * square))
        high, low = split(jnp.concatenate(parts, axis=1))
        turned = ((1,), (1,))
        res = (
            dot(high, high_ref[...], turned)
            + dot(low, high_ref[...], turned)
            + dot(high, low_ref[...], turned)
        )
        for dest, ref in enumerate(out_refs):
            ref[at, :] = res[:, dest * lanes : (dest + 1) * lanes]
        return carry

    lax.fori_loop(0, rows // ROWS, body, 0)


def y_inverse(*refs, count_py):
    x_refs, t_ref, out_refs = refs[:count_py], refs[count_py], refs[count_py + 1 :]
    table = t_ref[...]
    width, rows_y, _ = out_refs[0].shape

    def body(kz, carry):
        x = jnp.concatenate([ref[kz] for ref in x_refs], axis=0)
        res = left_apply(table, x)
        for dest, ref in enumerate(out_refs):
            ref[kz] = res[dest * rows_y : (dest + 1) * rows_y]
        return carry

    lax.fori_loop(0, width, body, 0, unroll=4)


def z_inverse(*refs, rows_y, count_pz, scale):
    *x_refs, c_ref, t_ref, out_ref = refs
    lanes = x_refs[0].shape[1]
    width = x_refs[0].shape[0] // rows_y
    chunks = len(x_refs) // count_pz
    table = t_ref[...]

    def body(y, carry):
        x = jnp.concatenate(
            [
                x_refs[n * count_pz + src][pl.ds(y, width, stride=rows_y), :]
                for src in range(count_pz)
                for n in range(chunks)
            ],
            axis=0,
        )
        high, low = split(x.T)
        res = dot(jnp.concatenate([high, high, low], axis=1), table)
        at = pl.ds(y, lanes, stride=rows_y)
        out_ref[at, :] = c_ref[at, :] - scale * res
        return carry

    lax.fori_loop(0, rows_y, body, 0, unroll=4)


VMEM = pl.BlockSpec(memory_space=pltpu.VMEM)
SMEM = pl.BlockSpec(memory_space=pltpu.SMEM)


def call(body, shapes, ins, specs=None, **kwargs):
    many = isinstance(shapes, list)
    listed = shapes if many else [shapes]
    out = pl.pallas_call(
        functools.partial(body, **kwargs),
        out_shape=[jax.ShapeDtypeStruct(s, F32) for s in listed],
        in_specs=specs or [VMEM] * len(ins),
        out_specs=[VMEM] * len(listed),
        name=body.__name__,
    )(*ins)
    return out if many else out[0]


def setting(concentration, mobility, kappa):
    species = concentration.shape[0]
    count_sp = lax.axis_size("sp")
    me = lax.axis_index("sp")
    own_kappa = lax.dynamic_slice_in_dim(kappa, me * species, species)
    columns = lax.dynamic_slice_in_dim(mobility, me * species, species, 1)
    shares = jnp.stack(
        [
            lax.dynamic_slice_in_dim(columns, (me + d) % count_sp * species, species, 0)
            for d in range(count_sp)
        ]
    )
    diagonal = lax.dynamic_slice_in_dim(jnp.diagonal(mobility), me * species, species)
    return own_kappa, shares, 0.5 * diagonal * own_kappa


def exchange(shares):
    count_sp = len(shares)
    out = [shares[0]]
    for d in range(1, count_sp):
        ring = [(i, (i + d) % count_sp) for i in range(count_sp)]
        out.append(lax.ppermute(shares[d], "sp", ring))
    return out


def swap(x, axis):
    return lax.all_to_all(x, axis, split_axis=0, concat_axis=0, tiled=True)


def hand_round(blocks, axis):
    count = len(blocks)
    out = [blocks[0]]
    for d in range(1, count):
        out.append(lax.ppermute(blocks[d], axis, [(i, (i - d) % count) for i in range(count)]))
    return out


def turn(table, *turns):
    starts, sizes = [0] * table.ndim, list(table.shape)
    for dimension, axis, step in turns:
        count = lax.axis_size(axis)
        block = table.shape[dimension] // count
        order = np.arange(2 * count - 1) * step % count
        places = (order[:, None] * block + np.arange(block)).reshape(-1)
        table = np.take(table, places, axis=dimension)
        starts[dimension] = lax.axis_index(axis) * step % count * block
    return lax.dynamic_slice(jnp.asarray(table), starts, sizes)


def dense(concentration, mobility, kappa, well_depth):
    species, rows_x, rows_y, depth = concentration.shape
    count_sp, count_py, count_pz = (lax.axis_size(a) for a in ("sp", "py", "pz"))
    full_x, full_y = rows_x * count_py, rows_y * count_pz
    lanes = species * rows_x
    narrow = full_y // count_py
    own_z = depth // count_pz
    chunks = CHUNKS
    width = own_z // chunks
    rows = width * narrow

    z_high, z_low = halves(cas_table(depth))
    y_high, y_low = halves(cas_table(full_y))
    z_left = turn(np.concatenate([z_high, z_low, z_high], axis=1), (0, "pz", -1))
    z_right = [turn(t, (0, "pz", 1)) for t in (z_high, z_low)]
    z_right = jnp.concatenate([*z_right, z_right[0]], axis=0)
    y_left = [turn(t, (1, "pz", 1), (0, "py", -1)) for t in (y_high, y_low)]
    y_left = jnp.concatenate([*y_left, y_left[0]], axis=1)
    y_back = [turn(t, (1, "py", 1), (0, "pz", -1)) for t in (y_high, y_low)]
    y_back = jnp.concatenate([*y_back, y_back[0]], axis=1)
    same = np.eye(species, dtype=bool)[None, :, None, :, None]

    def per_species(table):
        table = table.reshape(count_py, 1, rows_x, 1, full_x)
        return jnp.where(same, table, 0).reshape(count_py * lanes, species * full_x)

    x_tables = halves(cas_table(full_x))
    x_left = [per_species(turn(t, (0, "py", 1))) for t in x_tables]
    x_back = [per_species(turn(t, (0, "py", -1))) for t in x_tables]
    own_kappa, shares, stiff = setting(concentration, mobility, kappa)
    weight = jnp.broadcast_to(jnp.repeat(well_depth, rows_x)[:, None], (lanes, depth))
    flat = concentration.reshape(species * rows_x * rows_y, depth)
    ky = lax.axis_index("py") * narrow + jnp.arange(narrow, dtype=jnp.int32)
    ksq_x = wave_square(jnp.arange(full_x, dtype=jnp.int32), full_x)[None]

    spectra = call(
        z_forward,
        [(2, rows_y, width, lanes)] * (chunks * count_pz),
        (flat, weight, z_left),
        rows_y=rows_y,
        chunks=chunks,
    )
    moved = []
    for n in range(chunks):
        kz = lax.axis_index("pz") * own_z + n * width + jnp.arange(width, dtype=jnp.int32)
        ksq = wave_square(kz, depth)[:, None] + wave_square(ky, full_y)[None]
        ksq = jnp.broadcast_to(ksq.reshape(rows, 1), (rows, full_x))
        x = hand_round(spectra[n * count_pz : (n + 1) * count_pz], "pz")
        x = call(
            y_forward,
            [(2, width, narrow, lanes)] * count_py,
            (*[part.reshape(-1, lanes) for part in x], y_left),
            rows_y=rows_y,
            count_pz=count_pz,
        )
        x = hand_round(x, "py")
        mixes = call(
            x_forward,
            [(species, rows, full_x)] * count_sp,
            (*[part.reshape(2, rows, lanes) for part in x], *x_left, ksq, ksq_x, own_kappa, shares),
            [VMEM] * (count_py + 4) + [SMEM] * 2,
            sources=count_py,
        )
        mixes = exchange(mixes)
        x = call(
            x_inverse,
            [(rows, lanes)] * count_py,
            (*mixes, *x_back, ksq, ksq_x, stiff),
            [VMEM] * (count_sp + 4) + [SMEM],
            shares=count_sp,
        )
        x = hand_round(x, "py")
        x = call(
            y_inverse,
            [(width, rows_y, lanes)] * count_pz,
            (*[part.reshape(width, narrow, lanes) for part in x], y_back),
            count_py=count_py,
        )
        moved += [part.reshape(-1, lanes) for part in hand_round(x, "pz")]
    out = call(
        z_inverse,
        flat.shape,
        (*moved, flat, z_right),
        rows_y=rows_y,
        count_pz=count_pz,
        scale=1.0 / (full_x * full_y * depth),
    )
    return out.reshape(concentration.shape)


def contract(form, x, table):
    return jnp.einsum(form, x, table, precision=lax.Precision.HIGHEST)


def plain(concentration, mobility, kappa, well_depth):
    species, rows_x, rows_y, depth = concentration.shape
    count_py, count_pz = (lax.axis_size(a) for a in ("py", "pz"))
    full_x, full_y = rows_x * count_py, rows_y * count_pz
    narrow, own_z = full_y // count_py, depth // count_pz
    table_x, table_y, table_z = (jnp.asarray(cas_table(n), F32) for n in (full_x, full_y, depth))
    own_kappa, shares, stiff = setting(concentration, mobility, kappa)
    cube = concentration * concentration * concentration
    bulk = well_depth[:, None, None, None] * (cube - concentration)
    fields = jnp.stack([concentration, bulk])
    x = contract("fsxyz,kz->kfysx", fields, table_z)
    x = swap(x, "pz").reshape(count_pz, own_z, 2, rows_y, species, rows_x)
    x = contract("akfysx,qay->qfksx", x, table_y.reshape(full_y, count_pz, rows_y))
    x = swap(x, "py").reshape(count_py, narrow, 2, own_z, species, rows_x)
    x = contract("aqfksx,pax->fskqp", x, table_x.reshape(full_x, count_py, rows_x))
    kz = lax.axis_index("pz") * own_z + jnp.arange(own_z, dtype=jnp.int32)
    ky = lax.axis_index("py") * narrow + jnp.arange(narrow, dtype=jnp.int32)
    ksq_x = wave_square(jnp.arange(full_x, dtype=jnp.int32), full_x)
    ksq = wave_square(kz, depth)[:, None, None] + wave_square(ky, full_y)[:, None] + ksq_x
    drive = x[1] + own_kappa[:, None, None, None] * ksq * x[0]
    mixes = exchange([contract("skqp,is->ikqp", drive, shares[d]) for d in range(shares.shape[0])])
    x = 0.5 * ksq * sum(mixes) / (1.0 + stiff[:, None, None, None] * (ksq * ksq))
    x = swap(contract("skqp,xp->xqks", x, table_x), "py")
    x = x.reshape(count_py, rows_x, narrow, own_z, species)
    x = contract("axqks,yaq->yxks", x, table_y.reshape(full_y, count_py, narrow))
    x = swap(x, "pz").reshape(count_pz, rows_y, rows_x, own_z, species)
    x = contract("ayxks,zak->sxyz", x, table_z.reshape(depth, count_pz, own_z))
    return concentration - x * (1.0 / (full_x * full_y * depth))


def solution(mesh):
    def per_device(concentration, *rest):
        species, rows_x, rows_y, depth = concentration.shape
        full_x = rows_x * lax.axis_size("py")
        whole_tiles = [species * rows_x, full_x, depth]
        body = plain if any(n % 128 for n in whole_tiles) else dense
        return body(concentration, *rest)

    in_specs = (P("sp", "py", "pz", None), P(), P(), P("sp"))
    out_specs = P("sp", "py", "pz", None)
    return jax.shard_map(
        per_device, mesh=mesh, in_specs=in_specs, out_specs=out_specs, check_vma=False
    )
```
